16 devices in a mesh: rep: 4 (over y, z, core), pp: 4 (over x).
Axes of the slice: x: 4, y: 2, z: 1, core: 2. Of those that a mesh axis runs over, the one named last changes fastest.
The devices are a block of a 4x4x8 slice.
Arguments:
- x: bfloat16 [32, 512, 512], P('rep'), parts along dimension 0
- dy: bfloat16 [32, 512, 512], P('rep'), parts along dimension 0
- w_gate: bfloat16 [4, 512, 1792], P('pp')
- w_up: bfloat16 [4, 512, 1792], P('pp')
- w_down: bfloat16 [4, 1792, 512], P('pp')
Outputs:
- output 1: bfloat16 [16, 512, 1792], P(('rep', 'pp')), parts along dimension 0
- output 2: bfloat16 [16, 512, 1792], P(('rep', 'pp')), parts along dimension 0
- output 3: bfloat16 [16, 1792, 512], P(('rep', 'pp')), parts along dimension 0
There are 4 independent parts. The reference program is written for one: setup_inputs(seed, part) draws one part's arguments, and reference() takes and returns one part's arrays. A program takes and returns all parts, laid end to end along the dimension named above; an argument that names none is the same for every part.
All inputs are finite; a program needn't handle non-finite values.
Results may differ from the reference program's by a relative error of at most 0.018.
Values are sent between devices in bfloat16 or wider.
A program may use at most 768 MiB of HBM per device.

```python
import jax
import jax.numpy as jnp
from jax import lax

MICRO = 8
TOKENS = 512
D = 512
FF = 1792
LAYERS = 4
NAMES = ("w_gate", "w_up", "w_down")
SHAPES = {"w_gate": (LAYERS, D, FF), "w_up": (LAYERS, D, FF), "w_down": (LAYERS, FF, D)}


def bump(key, n, height):
    away = (jnp.arange(n, dtype=jnp.int32) - jax.random.randint(key, (), 0, n, jnp.int32)) % n
    return jnp.where(away < n // 8, height, 1.0)


def together(key, own, strength):
    shared = jax.random.normal(key, own.shape[1:], jnp.float32)
    return (own + strength * shared) * lax.rsqrt(1 + strength * strength)


def setup_inputs(seed: int = 0, part: int = 0) -> dict:
    kx, kdy, ka, kb, kz, kf, kh, kl, *kw = jax.random.split(jax.random.key(seed), 8 + len(NAMES))
    kx, kdy, ka, kb = (jax.random.fold_in(k, part) for k in (kx, kdy, ka, kb))
    shape = (MICRO, TOKENS, D)
    much_x, much_dy = jax.random.uniform(kz, (2,), jnp.float32, 0.0, 1.0)
    layers = 2.0 ** jax.random.uniform(kl, (LAYERS, 1, 1), jnp.float32, -1.0, 1.0)
    x = together(ka, jax.random.normal(kx, shape, jnp.float32), much_x) * bump(kf, D, 4.0)
    dy = together(kb, jax.random.normal(kdy, shape, jnp.float32), much_dy)
    drawn = {"x": x.astype(jnp.bfloat16), "dy": (dy * (MICRO * TOKENS) ** -0.5).astype(jnp.bfloat16)}
    for key, name in zip(kw, NAMES, strict=True):
        w = jax.random.normal(key, SHAPES[name], jnp.float32) * SHAPES[name][1] ** -0.5
        drawn[name] = (w * {"w_gate": 1.0, "w_up": bump(kh, FF, 4.0), "w_down": layers}[name]).astype(jnp.bfloat16)
    return drawn


def matmul(a, w):
    return jnp.dot(a, w, preferred_element_type=jnp.float32).astype(jnp.bfloat16)


def normed(h):
    wide = h.astype(jnp.float32)
    scale = lax.rsqrt(jnp.mean(wide**2, -1, keepdims=True) + 1e-6)
    return (wide * scale).astype(jnp.bfloat16)


def layer(h, w):
    a = normed(h)
    gate = jnp.dot(a, w["w_gate"], preferred_element_type=jnp.float32)
    up = jnp.dot(a, w["w_up"], preferred_element_type=jnp.float32)
    return h + matmul((jax.nn.silu(gate) * up).astype(jnp.bfloat16), w["w_down"])


def stack(weights, h):
    return lax.scan(lambda h, w: (layer(h, w), None), h, weights)[0]


def reference(x, dy, w_gate, w_up, w_down):
    weights = dict(zip(NAMES, (w_gate, w_up, w_down), strict=True))

    def take(so_far, one):
        h, by_y = one
        _, back = jax.vjp(lambda w: stack(w, h), weights)
        return jax.tree.map(lambda total, term: total + term.astype(jnp.float32), so_far, back(by_y)[0]), None

    none_yet = {name: jnp.zeros(w.shape, jnp.float32) for name, w in weights.items()}
    by_weights, _ = lax.scan(take, none_yet, (x, dy))
    return tuple(by_weights[name].astype(jnp.bfloat16) for name in NAMES)
```

```python
import functools

import jax
import jax.numpy as jnp
from jax import lax
from jax.experimental import pallas as pl
from jax.experimental.pallas import tpu as pltpu
from jax.sharding import PartitionSpec as P

ROWS = 128
COLS = 256
LAG = 4
MESH = pl.DeviceIdType.MESH
F32, BF16 = jnp.float32, jnp.bfloat16


def dot(a, b):
    return jnp.dot(a, b, preferred_element_type=F32)


def kernel(
    stages, pieces,
    x, dy, wg_in, wu_in, wd_in,
    og, ou, od,
    wg, wu, wd, wgt, wut, wdt, acc_g, acc_u, acc_d,
    h_in, d_in, h_out, d_out, act, dg, du, at, byt,
    w_sem, o_sem, rf, rb, sf, sb,
):
    me = lax.axis_index("pp")
    n, rows, d = x.shape
    ff = wg_in.shape[1]
    first, last = me == 0, me == stages - 1
    lag = (stages - 1 - me) * LAG

    def load_x(i):
        return pltpu.make_async_copy(x.at[i], h_in.at[i], rf.at[i])

    def load_dy(i):
        return pltpu.make_async_copy(dy.at[i], d_in.at[i], rb.at[i])

    weights = [
        pltpu.make_async_copy(src, dst, w_sem.at[k]) for k, (src, dst) in enumerate(((wg_in, wg), (wu_in, wu), (wd_in, wd)))
    ]

    @pl.when(first)
    def _():
        load_x(0).start()

    for w in weights:
        w.start()

    @pl.when(first)
    def _():
        lax.fori_loop(1, n, lambda i, c: (load_x(i).start(), c)[1], 0)

    @pl.when(last)
    def _():
        lax.fori_loop(0, n, lambda i, c: (load_dy(i).start(), c)[1], 0)

    def onward(i):
        return pltpu.make_async_remote_copy(
            src_ref=h_out.at[i], dst_ref=h_in.at[i], send_sem=sf.at[i], recv_sem=rf.at[i],
            device_id={"pp": jnp.minimum(me + 1, stages - 1)}, device_id_type=MESH,
        )

    def back(i):
        return pltpu.make_async_remote_copy(
            src_ref=d_out.at[i], dst_ref=d_in.at[i], send_sem=sb.at[i], recv_sem=rb.at[i],
            device_id={"pp": jnp.maximum(me - 1, 0)}, device_id_type=MESH,
        )

    barrier = pltpu.get_barrier_semaphore()

    @pl.when(me > 0)
    def _():
        pl.semaphore_signal(barrier, inc=1, device_id={"pp": me - 1}, device_id_type=MESH)

    @pl.when(me < stages - 1)
    def _():
        pl.semaphore_signal(barrier, inc=1, device_id={"pp": me + 1}, device_id_type=MESH)

    pl.semaphore_wait(barrier, (me > 0).astype(jnp.int32) + (me < stages - 1).astype(jnp.int32))

    for w in weights:
        w.wait()

    def wait_h(i):
        @pl.when(first)
        def _():
            load_x(i).wait()

        @pl.when(me > 0)
        def _():
            onward(i).wait_recv()

    def wait_d(i):
        @pl.when(last)
        def _():
            load_dy(i).wait()

        @pl.when(me < stages - 1)
        def _():
            back(i).wait_recv()

    def normed(i):
        wide = h_in[i].astype(F32)
        scale = lax.rsqrt(jnp.mean(wide * wide, -1, keepdims=True) + 1e-6)
        return wide, scale, (wide * scale).astype(BF16)

    def forward(i):
        wait_h(i)
        _, _, a = normed(i)
        for j in range(0, ff, COLS):
            cols = pl.ds(j, COLS)
            gate, up = dot(a, wg[:, cols]), dot(a, wu[:, cols])
            act[2, pl.ds(0, rows), cols] = (gate * jax.nn.sigmoid(gate) * up).astype(BF16)
        y = dot(act[2, pl.ds(0, rows), :], wd[...]).astype(BF16)
        h_out[i] = h_in[i] + y
        onward(i).start()

    def backward(i):
        @pl.when(last)
        def _():
            wait_h(i)

        wait_d(i)
        slot, c = lax.rem(lax.div(i, pieces), 2), lax.rem(i, pieces)
        here = pl.ds(pl.multiple_of(c * rows, rows), rows)
        wide, scale, a = normed(i)
        by = d_in[i]
        at[slot, :, here] = a.T
        byt[slot, :, here] = by.T
        for j in range(0, ff, COLS):
            cols = pl.ds(j, COLS)
            gate, up = dot(a, wg[:, cols]), dot(a, wu[:, cols])
            by_act = dot(by, wdt[:, cols]).astype(BF16).astype(F32)
            sg = jax.nn.sigmoid(gate)
            silu = gate * sg
            act[slot, here, cols] = (silu * up).astype(BF16)
            du[slot, here, cols] = (by_act * silu).astype(BF16)
            dg[slot, here, cols] = (by_act * up * (sg + silu * (1.0 - sg))).astype(BF16)

        @pl.when(me > 0)
        def _():
            by_a = dot(dg[slot, here, :], wgt[...]).astype(BF16) + dot(du[slot, here, :], wut[...]).astype(BF16)
            by_a = by_a.astype(F32)
            inner = jnp.sum(by_a * wide, -1, keepdims=True) * (scale * scale * scale) * (1.0 / d)
            d_out[i] = by + (by_a * scale - wide * inner).astype(BF16)
            back(i).start()

    def out_copies(slot, here, p):
        return [
            pltpu.make_async_copy(buf.at[slot, here, :], out.at[here, :], o_sem.at[k, p])
            for k, (buf, out) in enumerate(((dg, og), (du, ou), (act, od)))
        ]

    def weigh(i):
        m, p = lax.div(i, pieces), lax.rem(i, pieces)
        slot = lax.rem(m, 2)
        here = pl.ds(pl.multiple_of(p * (d // pieces), d // pieces), d // pieces)
        for left, right, acc in ((at, dg, acc_g), (at, du, acc_u), (byt, act, acc_d)):
            lhs = left[slot, here, :]
            for j in range(0, ff, COLS):
                cols = pl.ds(j, COLS)
                acc[here, cols] += dot(lhs, right[slot, :, cols]).astype(BF16).astype(F32)

        @pl.when(i >= n - pieces)
        def _():
            for acc, buf in ((acc_g, dg), (acc_u, du), (acc_d, act)):
                buf[1 - slot, here, :] = acc[here, :].astype(BF16)
            for copy in out_copies(1 - slot, here, p):
                copy.start()

    def step(i, carry):
        @pl.when((me < stages - 1) & (i < n))
        def _():
            forward(i)

        @pl.when(i == jnp.where(first, 1, 0))
        def _():
            for j in range(0, ff, COLS):
                wdt[:, j : j + COLS] = wd[j : j + COLS, :].T
            for acc in (acc_g, acc_u, acc_d):
                acc[...] = jnp.zeros_like(acc)

            @pl.when(me > 0)
            def _():
                for j in range(0, ff, COLS):
                    wgt[j : j + COLS, :] = wg[:, j : j + COLS].T
                    wut[j : j + COLS, :] = wu[:, j : j + COLS].T

        ib = i - lag

        @pl.when((ib >= 0) & (ib < n))
        def _():
            backward(ib)

        @pl.when(ib >= pieces)
        def _():
            weigh(ib - pieces)

        return carry

    lax.fori_loop(0, n + lag + pieces, step, 0)

    @pl.when(me < stages - 1)
    def _():
        lax.fori_loop(0, n, lambda i, c: (onward(i).wait_send(), c)[1], 0)

    @pl.when(me > 0)
    def _():
        lax.fori_loop(0, n, lambda i, c: (back(i).wait_send(), c)[1], 0)

    free = (n // pieces) % 2
    for p in range(pieces):
        for copy in out_copies(free, pl.ds(p * (d // pieces), d // pieces), p):
            copy.wait()


def solution(mesh):
    stages = mesh.shape["pp"]

    def step(x, dy, w_gate, w_up, w_down):
        micro, tokens, d = x.shape
        ff = w_gate.shape[2]
        pieces = tokens // ROWS
        n = micro * pieces
        chunks = lambda v: v.reshape(n, ROWS, d)
        vmem = lambda *shape, dtype=BF16: pltpu.VMEM(shape, dtype)
        sems = lambda *shape: pltpu.SemaphoreType.DMA(shape)
        og, ou, od = pl.pallas_call(
            functools.partial(kernel, stages, pieces),
            name="pipeline",
            out_shape=[jax.ShapeDtypeStruct((d, ff), BF16)] * 3,
            in_specs=[pl.BlockSpec(memory_space=pltpu.HBM)] * 5,
            out_specs=[pl.BlockSpec(memory_space=pltpu.HBM)] * 3,
            scratch_shapes=[
                vmem(d, ff), vmem(d, ff), vmem(ff, d), vmem(ff, d), vmem(ff, d), vmem(d, ff),
                *[vmem(d, ff, dtype=F32)] * 3,
                *[vmem(n, ROWS, d)] * 4,
                vmem(3, tokens, ff), vmem(2, tokens, ff), vmem(2, tokens, ff),
                vmem(2, d, tokens), vmem(2, d, tokens),
                sems(3), sems(3, pieces), sems(n), sems(n), sems(n), sems(n),
            ],
            compiler_params=pltpu.CompilerParams(collective_id=0, has_side_effects=True, vmem_limit_bytes=66_000_000),
        )(chunks(x), chunks(dy), w_gate[0], w_up[0], w_down[0])
        return og[None], ou[None], od.T[None]

    return jax.shard_map(
        step,
        mesh=mesh,
        in_specs=(P("rep", None, None),) * 2 + (P("pp", None, None),) * 3,
        out_specs=(P(("rep", "pp"), None, None),) * 3,
        check_vma=False,
    )
```

```python
import functools

import jax
import jax.numpy as jnp
from jax import lax
from jax.experimental import pallas as pl
from jax.experimental.pallas import tpu as pltpu
from jax.sharding import PartitionSpec as P

ROWS = 128
PARTS = 2
COLS = 256
RING = 8
LAG = 4
MESH = pl.DeviceIdType.MESH
F32, BF16 = jnp.float32, jnp.bfloat16


def dot(a, b):
    return jnp.dot(a, b, preferred_element_type=F32)


def kernel(
    stages, pieces,
    x, dy, wg_in, wu_in, wd_in,
    og, ou, od,
    wg, wu, wd, wgt, wut, wdt, acc_g, acc_u, acc_d,
    h_in, d_in, h_out, d_out, fact, kept_g, kept_u, act, dg, du, at, byt,
    w_sem, o_sem, rf, rb, sf, sb,
):
    me = lax.axis_index("pp")
    n, rows, d = x.shape
    ff = wg_in.shape[1]
    first, last = me == 0, me == stages - 1
    middle = (me > 0) & (me < stages - 1)
    keeps = kept_g.shape[0]
    lag = (stages - 1 - me) * LAG

    def load_x(i):
        return pltpu.make_async_copy(x.at[i], h_in.at[i], rf.at[i])

    def load_dy(i):
        return pltpu.make_async_copy(dy.at[i], d_in.at[i], rb.at[i])

    weights = [
        pltpu.make_async_copy(src, dst, w_sem.at[k]) for k, (src, dst) in enumerate(((wg_in, wg), (wu_in, wu), (wd_in, wd)))
    ]

    @pl.when(first)
    def _():
        load_x(0).start()

    for w in weights:
        w.start()

    @pl.when(first)
    def _():
        lax.fori_loop(1, n, lambda i, c: (load_x(i).start(), c)[1], 0)

    @pl.when(last)
    def _():
        lax.fori_loop(0, n, lambda i, c: (load_dy(i).start(), c)[1], 0)

    def onward(i):
        return pltpu.make_async_remote_copy(
            src_ref=h_out.at[lax.rem(i, RING)], dst_ref=h_in.at[i], send_sem=sf.at[i], recv_sem=rf.at[i],
            device_id={"pp": jnp.minimum(me + 1, stages - 1)}, device_id_type=MESH,
        )

    def back(i):
        return pltpu.make_async_remote_copy(
            src_ref=d_out.at[lax.rem(i, RING)], dst_ref=d_in.at[i], send_sem=sb.at[i], recv_sem=rb.at[i],
            device_id={"pp": jnp.maximum(me - 1, 0)}, device_id_type=MESH,
        )

    barrier = pltpu.get_barrier_semaphore()

    @pl.when(me > 0)
    def _():
        pl.semaphore_signal(barrier, inc=1, device_id={"pp": me - 1}, device_id_type=MESH)

    @pl.when(me < stages - 1)
    def _():
        pl.semaphore_signal(barrier, inc=1, device_id={"pp": me + 1}, device_id_type=MESH)

    pl.semaphore_wait(barrier, (me > 0).astype(jnp.int32) + (me < stages - 1).astype(jnp.int32))

    for w in weights:
        w.wait()

    def wait_h(i):
        @pl.when(first)
        def _():
            load_x(i).wait()

        @pl.when(me > 0)
        def _():
            onward(i).wait_recv()

    def wait_d(i):
        @pl.when(last)
        def _():
            load_dy(i).wait()

        @pl.when(me < stages - 1)
        def _():
            back(i).wait_recv()

    def normed(i):
        wide = h_in[i].astype(F32)
        scale = lax.rsqrt(jnp.mean(wide * wide, -1, keepdims=True) + 1e-6)
        return wide, scale, (wide * scale).astype(BF16)

    def forward(i):
        wait_h(i)

        @pl.when(i >= RING)
        def _():
            onward(i - RING).wait_send()

        _, _, a = normed(i)
        spot = lax.rem(i, keeps)
        for j in range(0, ff, COLS):
            cols = pl.ds(j, COLS)
            gate, up = dot(a, wg[:, cols]), dot(a, wu[:, cols])
            kept_g[spot, :, cols] = gate
            kept_u[spot, :, cols] = up
            fact[:, cols] = (gate * jax.nn.sigmoid(gate) * up).astype(BF16)
        y = dot(fact[...], wd[...]).astype(BF16)
        h_out[lax.rem(i, RING)] = h_in[i] + y
        onward(i).start()

    def backward(i, recompute):
        @pl.when(last)
        def _():
            wait_h(i)

        wait_d(i)
        slot, c = lax.rem(lax.div(i, pieces), 2), lax.rem(i, pieces)
        here = pl.ds(pl.multiple_of(c * rows, rows), rows)
        spot = lax.rem(i, keeps)
        wide, scale, a = normed(i)
        by = d_in[i]
        at[slot, :, here] = a.T
        byt[slot, :, here] = by.T
        for j in range(0, ff, COLS):
            cols = pl.ds(j, COLS)
            if recompute:
                gate, up = dot(a, wg[:, cols]), dot(a, wu[:, cols])
            else:
                gate, up = kept_g[spot, :, cols], kept_u[spot, :, cols]
            by_act = dot(by, wdt[:, cols]).astype(BF16).astype(F32)
            sg = jax.nn.sigmoid(gate)
            silu = gate * sg
            act[slot, here, cols] = (silu * up).astype(BF16)
            du[slot, here, cols] = (by_act * silu).astype(BF16)
            dg[slot, here, cols] = (by_act * up * (sg + silu * (1.0 - sg))).astype(BF16)

        def send():
            @pl.when(i >= RING)
            def _():
                back(i - RING).wait_send()

            by_a = dot(dg[slot, here, :], wgt[...]).astype(BF16) + dot(du[slot, here, :], wut[...]).astype(BF16)
            by_a = by_a.astype(F32)
            inner = jnp.sum(by_a * wide, -1, keepdims=True) * (scale * scale * scale) * (1.0 / d)
            d_out[lax.rem(i, RING)] = by + (by_a * scale - wide * inner).astype(BF16)
            back(i).start()

        pl.when(me > 0)(send) if recompute else send()

    def out_copies(slot, p):
        here = pl.ds(p * (d // PARTS), d // PARTS)
        return [
            pltpu.make_async_copy(buf.at[slot, here, :], out.at[here, :], o_sem.at[k, p])
            for k, (buf, out) in enumerate(((dg, og), (du, ou), (act, od)))
        ]

    def weigh(m, p):
        slot = lax.rem(m, 2)
        here = pl.ds(pl.multiple_of(p * (d // PARTS), d // PARTS), d // PARTS)
        for left, right, acc in ((at, dg, acc_g), (at, du, acc_u), (byt, act, acc_d)):
            lhs = left[slot, here, :]
            for j in range(0, ff, COLS):
                cols = pl.ds(j, COLS)
                acc[here, cols] += dot(lhs, right[slot, :, cols]).astype(BF16).astype(F32)

        @pl.when(m == n // pieces - 1)
        def _():
            for acc, buf in ((acc_g, dg), (acc_u, du), (acc_d, act)):
                buf[1 - slot, here, :] = acc[here, :].astype(BF16)
            for copy in out_copies(1 - slot, p):
                copy.start()

    def step(i, carry):
        @pl.when((me < stages - 1) & (i < n))
        def _():
            forward(i)

        @pl.when(i == jnp.where(first, 1, 0))
        def _():
            for j in range(0, ff, COLS):
                wdt[:, j : j + COLS] = wd[j : j + COLS, :].T
            for acc in (acc_g, acc_u, acc_d):
                acc[...] = jnp.zeros_like(acc)

            @pl.when(me > 0)
            def _():
                for j in range(0, ff, COLS):
                    wgt[j : j + COLS, :] = wg[:, j : j + COLS].T
                    wut[j : j + COLS, :] = wu[:, j : j + COLS].T

        ib = i - lag

        @pl.when((ib >= 0) & (ib < n) & middle)
        def _():
            backward(ib, False)

        @pl.when((ib >= 0) & (ib < n) & ~middle)
        def _():
            backward(ib, True)

        iw, every = ib - pieces, pieces // PARTS

        @pl.when((iw >= 0) & (lax.rem(iw + pieces, every) == every - 1))
        def _():
            weigh(lax.div(iw, pieces), lax.div(lax.rem(iw, pieces), every))

        return carry

    lax.fori_loop(0, n + lag + pieces, step, 0)

    @pl.when(me < stages - 1)
    def _():
        lax.fori_loop(n - RING, n, lambda i, c: (onward(i).wait_send(), c)[1], 0)

    @pl.when(me > 0)
    def _():
        lax.fori_loop(n - RING, n, lambda i, c: (back(i).wait_send(), c)[1], 0)

    free = (n // pieces) % 2
    for p in range(PARTS):
        for copy in out_copies(free, p):
            copy.wait()


def solution(mesh):
    stages = mesh.shape["pp"]

    def step(x, dy, w_gate, w_up, w_down):
        micro, tokens, d = x.shape
        ff = w_gate.shape[2]
        pieces = tokens // ROWS
        n = micro * pieces
        chunks = lambda v: v.reshape(n, ROWS, d)
        vmem = lambda *shape, dtype=BF16: pltpu.VMEM(shape, dtype)
        sems = lambda *shape: pltpu.SemaphoreType.DMA(shape)
        og, ou, od = pl.pallas_call(
            functools.partial(kernel, stages, pieces),
            name="pipeline",
            out_shape=[jax.ShapeDtypeStruct((d, ff), BF16)] * 3,
            in_specs=[pl.BlockSpec(memory_space=pltpu.HBM)] * 5,
            out_specs=[pl.BlockSpec(memory_space=pltpu.HBM)] * 3,
            scratch_shapes=[
                vmem(d, ff), vmem(d, ff), vmem(ff, d), vmem(ff, d), vmem(ff, d), vmem(d, ff),
                *[vmem(d, ff, dtype=F32)] * 3,
                *[vmem(n, ROWS, d)] * 2,
                *[vmem(RING, ROWS, d)] * 2,
                vmem(ROWS, ff),
                *[vmem(max(stages - 2, 0) * LAG + 1, ROWS, ff, dtype=F32)] * 2,
                *[vmem(2, tokens, ff)] * 3,
                vmem(2, d, tokens), vmem(2, d, tokens),
                sems(3), sems(3, PARTS), sems(n), sems(n), sems(n), sems(n),
            ],
            compiler_params=pltpu.CompilerParams(collective_id=0, has_side_effects=True, vmem_limit_bytes=67_000_000),
        )(chunks(x), chunks(dy), w_gate[0], w_up[0], w_down[0])
        return og[None], ou[None], od.T[None]

    return jax.shard_map(
        step,
        mesh=mesh,
        in_specs=(P("rep", None, None),) * 2 + (P("pp", None, None),) * 3,
        out_specs=(P(("rep", "pp"), None, None),) * 3,
        check_vma=False,
    )
```

```python
import functools

import jax
import jax.numpy as jnp
from jax import lax
from jax.experimental import pallas as pl
from jax.experimental.pallas import tpu as pltpu
from jax.sharding import PartitionSpec as P

ROWS = 128
PARTS = 2
COLS = 256
RING = 8
LAG = 4
MESH = pl.DeviceIdType.MESH
F32, BF16 = jnp.float32, jnp.bfloat16


def dot(a, b):
    return jnp.dot(a, b, preferred_element_type=F32)


def kernel(
    stages, pieces,
    x, dy, wg_in, wu_in, wd_in,
    wg, wu, wd,
    wgt, wut, wdt, acc_g, acc_u, acc_d,
    h_in, d_in, h_out, d_out, kept_g, kept_u, act, dg, du, at, byt,
    w_sem, rf, rb, sf, sb,
):
    me = lax.axis_index("pp")
    n, rows, d = x.shape
    ff = wg_in.shape[1]
    first, last = me == 0, me == stages - 1
    middle = (me > 0) & (me < stages - 1)
    keeps = kept_g.shape[0]
    lag = (stages - 1 - me) * LAG

    def load_x(i):
        return pltpu.make_async_copy(x.at[i], h_in.at[i], rf.at[i])

    def load_dy(i):
        return pltpu.make_async_copy(dy.at[i], d_in.at[i], rb.at[i])

    weights = [
        pltpu.make_async_copy(src, dst, w_sem.at[k]) for k, (src, dst) in enumerate(((wg_in, wg), (wu_in, wu), (wd_in, wd)))
    ]

    @pl.when(first)
    def _():
        load_x(0).start()

    for w in weights:
        w.start()

    @pl.when(first)
    def _():
        lax.fori_loop(1, n, lambda i, c: (load_x(i).start(), c)[1], 0)

    @pl.when(last)
    def _():
        lax.fori_loop(0, n, lambda i, c: (load_dy(i).start(), c)[1], 0)

    def onward(i):
        return pltpu.make_async_remote_copy(
            src_ref=h_out.at[lax.rem(i, RING)], dst_ref=h_in.at[i], send_sem=sf.at[i], recv_sem=rf.at[i],
            device_id={"pp": jnp.minimum(me + 1, stages - 1)}, device_id_type=MESH,
        )

    def back(i):
        return pltpu.make_async_remote_copy(
            src_ref=d_out.at[lax.rem(i, RING)], dst_ref=d_in.at[i], send_sem=sb.at[i], recv_sem=rb.at[i],
            device_id={"pp": jnp.maximum(me - 1, 0)}, device_id_type=MESH,
        )

    barrier = pltpu.get_barrier_semaphore()

    @pl.when(me > 0)
    def _():
        pl.semaphore_signal(barrier, inc=1, device_id={"pp": me - 1}, device_id_type=MESH)

    @pl.when(me < stages - 1)
    def _():
        pl.semaphore_signal(barrier, inc=1, device_id={"pp": me + 1}, device_id_type=MESH)

    pl.semaphore_wait(barrier, (me > 0).astype(jnp.int32) + (me < stages - 1).astype(jnp.int32))

    for w in weights:
        w.wait()

    def wait_h(i):
        @pl.when(first)
        def _():
            load_x(i).wait()

        @pl.when(me > 0)
        def _():
            onward(i).wait_recv()

    def wait_d(i):
        @pl.when(last)
        def _():
            load_dy(i).wait()

        @pl.when(me < stages - 1)
        def _():
            back(i).wait_recv()

    def normed(i):
        wide = h_in[i].astype(F32)
        scale = lax.rsqrt(jnp.mean(wide * wide, -1, keepdims=True) + 1e-6)
        return wide, scale, (wide * scale).astype(BF16)

    def forward(i):
        wait_h(i)

        @pl.when(i >= RING)
        def _():
            onward(i - RING).wait_send()

        _, _, a = normed(i)
        spot = lax.rem(i, keeps)
        y = 0.0
        for j in range(0, ff, COLS):
            cols = pl.ds(j, COLS)
            gate, up = dot(a, wg[:, cols]), dot(a, wu[:, cols])
            kept_g[spot, :, cols] = gate
            kept_u[spot, :, cols] = up
            y += dot((gate * jax.nn.sigmoid(gate) * up).astype(BF16), wd[cols, :])
        y = y.astype(BF16)
        h_out[lax.rem(i, RING)] = h_in[i] + y
        onward(i).start()

    def backward(i, recompute, send):
        @pl.when(last)
        def _():
            wait_h(i)

        wait_d(i)
        slot, c = lax.rem(lax.div(i, pieces), 2), lax.rem(i, pieces)
        here = pl.ds(pl.multiple_of(c * rows, rows), rows)
        spot = lax.rem(i, keeps)
        if send:

            @pl.when(i >= RING)
            def _():
                back(i - RING).wait_send()

        wide, scale, a = normed(i)
        by = d_in[i]
        at[slot, :, here] = a.T
        byt[slot, :, here] = by.T
        by_a_g, by_a_u = 0.0, 0.0
        for j in range(0, ff, COLS):
            cols = pl.ds(j, COLS)
            if recompute:
                gate, up = dot(a, wg[:, cols]), dot(a, wu[:, cols])
            else:
                gate, up = kept_g[spot, :, cols], kept_u[spot, :, cols]
            by_act = dot(by, wdt[:, cols]).astype(BF16).astype(F32)
            sg = jax.nn.sigmoid(gate)
            silu = gate * sg
            by_up = (by_act * silu).astype(BF16)
            by_gate = (by_act * up * (sg + silu * (1.0 - sg))).astype(BF16)
            act[slot, here, cols] = (silu * up).astype(BF16)
            du[slot, here, cols] = by_up
            dg[slot, here, cols] = by_gate
            if send:
                by_a_g += dot(by_gate, wgt[cols, :])
                by_a_u += dot(by_up, wut[cols, :])
        if send:
            by_a = (by_a_g.astype(BF16) + by_a_u.astype(BF16)).astype(F32)
            inner = jnp.sum(by_a * wide, -1, keepdims=True) * (scale * scale * scale) * (1.0 / d)
            d_out[lax.rem(i, RING)] = by + (by_a * scale - wide * inner).astype(BF16)
            back(i).start()

    def weigh(m, p, final):
        slot = lax.rem(m, 2)
        here = pl.ds(pl.multiple_of(p * (d // PARTS), d // PARTS), d // PARTS)
        for left, right, acc, out in ((at, dg, acc_g, wg), (at, du, acc_u, wu), (byt, act, acc_d, wd)):
            lhs = left[slot, here, :]
            for j in range(0, ff, COLS):
                cols = pl.ds(j, COLS)
                total = acc[here, cols] + dot(lhs, right[slot, :, cols]).astype(BF16).astype(F32)
                if not final:
                    acc[here, cols] = total
                elif out is wd:
                    out[cols, here] = total.astype(BF16).T
                else:
                    out[here, cols] = total.astype(BF16)

    def step(i, carry):
        @pl.when(i == jnp.where(first, 2, 0))
        def _():
            for j in range(0, ff, COLS):
                wdt[:, j : j + COLS] = wd[j : j + COLS, :].T
            for acc in (acc_g, acc_u, acc_d):
                acc[...] = jnp.zeros_like(acc)

            @pl.when(me > 0)
            def _():
                for j in range(0, ff, COLS):
                    wgt[j : j + COLS, :] = wg[:, j : j + COLS].T
                    wut[j : j + COLS, :] = wu[:, j : j + COLS].T

        @pl.when((me < stages - 1) & (i < n))
        def _():
            forward(i)

        ib = i - lag

        @pl.when((ib >= 0) & (ib < n) & middle)
        def _():
            backward(ib, False, True)

        @pl.when((ib >= 0) & (ib < n) & last)
        def _():
            backward(ib, True, True)

        @pl.when((ib >= 0) & (ib < n) & first)
        def _():
            backward(ib, True, False)

        iw, every = ib - pieces, pieces // PARTS
        turn = (iw >= 0) & (lax.rem(iw + pieces, every) == every - 1)
        mw, pw = lax.div(iw, pieces), lax.div(lax.rem(iw, pieces), every)

        @pl.when(turn & (iw < n - pieces))
        def _():
            weigh(mw, pw, False)

        @pl.when(turn & (iw >= n - pieces))
        def _():
            weigh(mw, pw, True)

        return carry

    lax.fori_loop(0, n + lag + pieces, step, 0)

    @pl.when(me < stages - 1)
    def _():
        lax.fori_loop(n - RING, n, lambda i, c: (onward(i).wait_send(), c)[1], 0)

    @pl.when(me > 0)
    def _():
        lax.fori_loop(n - RING, n, lambda i, c: (back(i).wait_send(), c)[1], 0)


def solution(mesh):
    stages = mesh.shape["pp"]

    def step(x, dy, w_gate, w_up, w_down):
        micro, tokens, d = x.shape
        ff = w_gate.shape[2]
        pieces = tokens // ROWS
        n = micro * pieces
        chunks = lambda v: v.reshape(n, ROWS, d)
        vmem = lambda *shape, dtype=BF16: pltpu.VMEM(shape, dtype)
        sems = lambda *shape: pltpu.SemaphoreType.DMA(shape)
        og, ou, od = pl.pallas_call(
            functools.partial(kernel, stages, pieces),
            name="pipeline",
            out_shape=[pltpu.VMEM(shape, BF16) for shape in ((d, ff), (d, ff), (ff, d))],
            in_specs=[pl.BlockSpec(memory_space=pltpu.HBM)] * 5,
            out_specs=[pl.BlockSpec(memory_space=pltpu.VMEM)] * 3,
            scratch_shapes=[
                vmem(ff, d), vmem(ff, d), vmem(d, ff),
                *[vmem(d, ff, dtype=F32)] * 3,
                *[vmem(n, ROWS, d)] * 2,
                *[vmem(RING, ROWS, d)] * 2,
                *[vmem(max(stages - 2, 0) * LAG + 1, ROWS, ff, dtype=F32)] * 2,
                *[vmem(2, tokens, ff)] * 3,
                vmem(2, d, tokens), vmem(2, d, tokens),
                sems(3), sems(n), sems(n), sems(n), sems(n),
            ],
            compiler_params=pltpu.CompilerParams(collective_id=0, has_side_effects=True, vmem_limit_bytes=60_500_000),
        )(chunks(x), chunks(dy), w_gate[0], w_up[0], w_down[0])
        return og[None], ou[None], od[None]

    return jax.shard_map(
        step,
        mesh=mesh,
        in_specs=(P("rep", None, None),) * 2 + (P("pp", None, None),) * 3,
        out_specs=(P(("rep", "pp"), None, None),) * 3,
        check_vma=False,
    )
```

```python
import functools

import jax
import jax.numpy as jnp
from jax import lax
from jax.experimental import pallas as pl
from jax.experimental.pallas import tpu as pltpu
from jax.sharding import PartitionSpec as P

ROWS = 128
PARTS = 2
COLS = 256
RING = 8
LAG = 4
MESH = pl.DeviceIdType.MESH
F32, BF16 = jnp.float32, jnp.bfloat16


def dot(a, b):
    return jnp.dot(a, b, preferred_element_type=F32)


def kernel(
    stages, pieces,
    x, dy, wg_in, wu_in, wd_in,
    wg, wu, wd,
    wgt, wut, wdt, acc_g, acc_u, acc_d,
    h_in, d_in, h_out, d_out, fact, kept_g, kept_u, act, dg, du, at, byt,
    w_sem, rf, rb, sf, sb,
):
    me = lax.axis_index("pp")
    n, rows, d = x.shape
    ff = wg_in.shape[1]
    first, last = me == 0, me == stages - 1
    middle = (me > 0) & (me < stages - 1)
    keeps = kept_g.shape[0]
    lag = (stages - 1 - me) * LAG

    def load_x(i):
        return pltpu.make_async_copy(x.at[i], h_in.at[i], rf.at[i])

    def load_dy(i):
        return pltpu.make_async_copy(dy.at[i], d_in.at[i], rb.at[i])

    weights = [
        pltpu.make_async_copy(src, dst, w_sem.at[k]) for k, (src, dst) in enumerate(((wg_in, wg), (wu_in, wu), (wd_in, wd)))
    ]

    @pl.when(first)
    def _():
        load_x(0).start()

    for w in weights:
        w.start()

    @pl.when(first)
    def _():
        lax.fori_loop(1, n, lambda i, c: (load_x(i).start(), c)[1], 0)

    @pl.when(last)
    def _():
        lax.fori_loop(0, n, lambda i, c: (load_dy(i).start(), c)[1], 0)

    def onward(i):
        return pltpu.make_async_remote_copy(
            src_ref=h_out.at[lax.rem(i, RING)], dst_ref=h_in.at[i], send_sem=sf.at[i], recv_sem=rf.at[i],
            device_id={"pp": jnp.minimum(me + 1, stages - 1)}, device_id_type=MESH,
        )

    def back(i):
        return pltpu.make_async_remote_copy(
            src_ref=d_out.at[lax.rem(i, RING)], dst_ref=d_in.at[i], send_sem=sb.at[i], recv_sem=rb.at[i],
            device_id={"pp": jnp.maximum(me - 1, 0)}, device_id_type=MESH,
        )

    barrier = pltpu.get_barrier_semaphore()

    @pl.when(me > 0)
    def _():
        pl.semaphore_signal(barrier, inc=1, device_id={"pp": me - 1}, device_id_type=MESH)

    @pl.when(me < stages - 1)
    def _():
        pl.semaphore_signal(barrier, inc=1, device_id={"pp": me + 1}, device_id_type=MESH)

    pl.semaphore_wait(barrier, (me > 0).astype(jnp.int32) + (me < stages - 1).astype(jnp.int32))

    for w in weights:
        w.wait()

    def wait_h(i):
        @pl.when(first)
        def _():
            load_x(i).wait()

        @pl.when(me > 0)
        def _():
            onward(i).wait_recv()

    def wait_d(i):
        @pl.when(last)
        def _():
            load_dy(i).wait()

        @pl.when(me < stages - 1)
        def _():
            back(i).wait_recv()

    def normed(i):
        wide = h_in[i].astype(F32)
        scale = lax.rsqrt(jnp.mean(wide * wide, -1, keepdims=True) + 1e-6)
        return wide, scale, (wide * scale).astype(BF16)

    def forward(i):
        wait_h(i)

        @pl.when(i >= RING)
        def _():
            onward(i - RING).wait_send()

        _, _, a = normed(i)
        spot = lax.rem(i, keeps)
        for j in range(0, ff, COLS):
            cols = pl.ds(j, COLS)
            gate, up = dot(a, wg[:, cols]), dot(a, wu[:, cols])
            kept_g[spot, :, cols] = gate
            kept_u[spot, :, cols] = up
            fact[:, cols] = (gate * jax.nn.sigmoid(gate) * up).astype(BF16)
        y = dot(fact[...], wd[...]).astype(BF16)
        h_out[lax.rem(i, RING)] = h_in[i] + y
        onward(i).start()

    def backward(i, recompute, send):
        @pl.when(last)
        def _():
            wait_h(i)

        wait_d(i)
        slot, c = lax.rem(lax.div(i, pieces), 2), lax.rem(i, pieces)
        here = pl.ds(pl.multiple_of(c * rows, rows), rows)
        spot = lax.rem(i, keeps)
        if send:

            @pl.when(i >= RING)
            def _():
                back(i - RING).wait_send()

        wide, scale, a = normed(i)
        by = d_in[i]
        at[slot, :, here] = a.T
        byt[slot, :, here] = by.T
        firsts = []
        for j in range(0, ff, COLS):
            cols = pl.ds(j, COLS)
            gate_up = (dot(a, wg[:, cols]), dot(a, wu[:, cols])) if recompute else ()
            firsts.append((*gate_up, dot(by, wdt[:, cols])))
        by_a_g, by_a_u = 0.0, 0.0
        for j, (*gate_up, by_act) in zip(range(0, ff, COLS), firsts, strict=True):
            cols = pl.ds(j, COLS)
            gate, up = gate_up if recompute else (kept_g[spot, :, cols], kept_u[spot, :, cols])
            by_act = by_act.astype(BF16).astype(F32)
            sg = jax.nn.sigmoid(gate)
            silu = gate * sg
            by_up = (by_act * silu).astype(BF16)
            by_gate = (by_act * up * (sg + silu * (1.0 - sg))).astype(BF16)
            act[slot, here, cols] = (silu * up).astype(BF16)
            du[slot, here, cols] = by_up
            dg[slot, here, cols] = by_gate
            if send:
                by_a_g += dot(by_gate, wgt[cols, :])
                by_a_u += dot(by_up, wut[cols, :])
        if send:
            by_a = (by_a_g.astype(BF16) + by_a_u.astype(BF16)).astype(F32)
            inner = jnp.sum(by_a * wide, -1, keepdims=True) * (scale * scale * scale) * (1.0 / d)
            d_out[lax.rem(i, RING)] = by + (by_a * scale - wide * inner).astype(BF16)
            back(i).start()

    def weigh(m, p, final):
        slot = lax.rem(m, 2)
        here = pl.ds(pl.multiple_of(p * (d // PARTS), d // PARTS), d // PARTS)
        for left, right, acc, out in ((at, dg, acc_g, wg), (at, du, acc_u, wu), (byt, act, acc_d, wd)):
            lhs = left[slot, here, :]
            for j in range(0, ff, COLS):
                cols = pl.ds(j, COLS)
                total = acc[here, cols] + dot(lhs, right[slot, :, cols]).astype(BF16).astype(F32)
                if not final:
                    acc[here, cols] = total
                elif out is wd:
                    out[cols, here] = total.astype(BF16).T
                else:
                    out[here, cols] = total.astype(BF16)

    def step(i, carry):
        @pl.when(i == jnp.where(first, 2, 0))
        def _():
            for j in range(0, ff, COLS):
                wdt[:, j : j + COLS] = wd[j : j + COLS, :].T
            for acc in (acc_g, acc_u, acc_d):
                acc[...] = jnp.zeros_like(acc)

            @pl.when(me > 0)
            def _():
                for j in range(0, ff, COLS):
                    wgt[j : j + COLS, :] = wg[:, j : j + COLS].T
                    wut[j : j + COLS, :] = wu[:, j : j + COLS].T

        @pl.when((me < stages - 1) & (i < n))
        def _():
            forward(i)

        ib = i - lag

        @pl.when((ib >= 0) & (ib < n) & middle)
        def _():
            backward(ib, False, True)

        @pl.when((ib >= 0) & (ib < n) & last)
        def _():
            backward(ib, True, True)

        @pl.when((ib >= 0) & (ib < n) & first)
        def _():
            backward(ib, True, False)

        iw, every = ib - pieces, pieces // PARTS
        turn = (iw >= 0) & (lax.rem(iw + pieces, every) == every - 1)
        mw, pw = lax.div(iw, pieces), lax.div(lax.rem(iw, pieces), every)

        @pl.when(turn & (iw < n - pieces))
        def _():
            weigh(mw, pw, False)

        @pl.when(turn & (iw >= n - pieces))
        def _():
            weigh(mw, pw, True)

        return carry

    lax.fori_loop(0, n + lag + pieces, step, 0)

    @pl.when(me < stages - 1)
    def _():
        lax.fori_loop(n - RING, n, lambda i, c: (onward(i).wait_send(), c)[1], 0)

    @pl.when(me > 0)
    def _():
        lax.fori_loop(n - RING, n, lambda i, c: (back(i).wait_send(), c)[1], 0)


def solution(mesh):
    stages = mesh.shape["pp"]

    def step(x, dy, w_gate, w_up, w_down):
        micro, tokens, d = x.shape
        ff = w_gate.shape[2]
        pieces = tokens // ROWS
        n = micro * pieces
        chunks = lambda v: v.reshape(n, ROWS, d)
        vmem = lambda *shape, dtype=BF16: pltpu.VMEM(shape, dtype)
        sems = lambda *shape: pltpu.SemaphoreType.DMA(shape)
        og, ou, od = pl.pallas_call(
            functools.partial(kernel, stages, pieces),
            name="pipeline",
            out_shape=[pltpu.VMEM(shape, BF16) for shape in ((d, ff), (d, ff), (ff, d))],
            in_specs=[pl.BlockSpec(memory_space=pltpu.HBM)] * 5,
            out_specs=[pl.BlockSpec(memory_space=pltpu.VMEM)] * 3,
            scratch_shapes=[
                vmem(ff, d), vmem(ff, d), vmem(d, ff),
                *[vmem(d, ff, dtype=F32)] * 3,
                *[vmem(n, ROWS, d)] * 2,
                *[vmem(RING, ROWS, d)] * 2,
                vmem(ROWS, ff),
                *[vmem(max(stages - 2, 0) * LAG + 1, ROWS, ff, dtype=F32)] * 2,
                *[vmem(2, tokens, ff)] * 3,
                vmem(2, d, tokens), vmem(2, d, tokens),
                sems(3), sems(n), sems(n), sems(n), sems(n),
            ],
            compiler_params=pltpu.CompilerParams(collective_id=0, has_side_effects=True, vmem_limit_bytes=60_500_000),
        )(chunks(x), chunks(dy), w_gate[0], w_up[0], w_down[0])
        return og[None], ou[None], od[None]

    return jax.shard_map(
        step,
        mesh=mesh,
        in_specs=(P("rep", None, None),) * 2 + (P("pp", None, None),) * 3,
        out_specs=(P(("rep", "pp"), None, None),) * 3,
        check_vma=False,
    )
```

```python
import functools

import jax
import jax.numpy as jnp
from jax import lax
from jax.experimental import pallas as pl
from jax.experimental.pallas import tpu as pltpu
from jax.sharding import PartitionSpec as P

ROWS = 128
PARTS = 2
COLS = 256
RING = 3
LAG = 4
MESH = pl.DeviceIdType.MESH
F32, BF16 = jnp.float32, jnp.bfloat16


def dot(a, b):
    return jnp.dot(a, b, preferred_element_type=F32)


def kernel(
    stages, pieces,
    x, dy, wg_in, wu_in, wd_in,
    wg, wu, wd,
    wgt, wut, wdt, acc_g, acc_u, acc_d,
    h_in, d_in, h_out, kept_s, kept_q, act, dg, du, at, byt,
    w_sem, rf, rb, sf, sb,
):
    me = lax.axis_index("pp")
    n, rows, d = x.shape
    ff = wg_in.shape[1]
    first, last = me == 0, me == stages - 1
    middle = (me > 0) & (me < stages - 1)
    keeps = kept_s.shape[0]
    lag = (stages - 1 - me) * LAG

    def load_x(i):
        return pltpu.make_async_copy(x.at[i], h_in.at[i], rf.at[i])

    def load_dy(i):
        return pltpu.make_async_copy(dy.at[i], d_in.at[i], rb.at[i])

    tiles = range(0, ff, COLS)

    def load_w(k, j):
        src, dst = ((wg_in, wg), (wu_in, wu), (wd_in, wd))[k]
        part = (pl.ds(j, COLS), slice(None)) if k == 2 else (slice(None), pl.ds(j, COLS))
        return pltpu.make_async_copy(src.at[part], dst.at[part], w_sem.at[k, j // COLS])

    @pl.when(first)
    def _():
        load_x(0).start()

    for j in tiles:
        load_w(0, j).start()
        load_w(1, j).start()
    for j in tiles:
        load_w(2, j).start()

    @pl.when(first)
    def _():
        lax.fori_loop(1, n, lambda i, c: (load_x(i).start(), c)[1], 0)

    @pl.when(last)
    def _():
        lax.fori_loop(0, n, lambda i, c: (load_dy(i).start(), c)[1], 0)

    def onward(i):
        return pltpu.make_async_remote_copy(
            src_ref=h_out.at[lax.rem(i, RING)], dst_ref=h_in.at[i], send_sem=sf.at[i], recv_sem=rf.at[i],
            device_id={"pp": jnp.minimum(me + 1, stages - 1)}, device_id_type=MESH,
        )

    def back(i):
        return pltpu.make_async_remote_copy(
            src_ref=d_in.at[i], dst_ref=d_in.at[i], send_sem=sb.at[i], recv_sem=rb.at[i],
            device_id={"pp": jnp.maximum(me - 1, 0)}, device_id_type=MESH,
        )

    barrier = pltpu.get_barrier_semaphore()

    @pl.when(me > 0)
    def _():
        pl.semaphore_signal(barrier, inc=1, device_id={"pp": me - 1}, device_id_type=MESH)

    @pl.when(me < stages - 1)
    def _():
        pl.semaphore_signal(barrier, inc=1, device_id={"pp": me + 1}, device_id_type=MESH)

    pl.semaphore_wait(barrier, (me > 0).astype(jnp.int32) + (me < stages - 1).astype(jnp.int32))

    @pl.when(me > 0)
    def _():
        for j in tiles:
            for k in range(3):
                load_w(k, j).wait()

    def wait_h(i):
        @pl.when(first)
        def _():
            load_x(i).wait()

        @pl.when(me > 0)
        def _():
            onward(i).wait_recv()

    def wait_d(i):
        @pl.when(last)
        def _():
            load_dy(i).wait()

        @pl.when(me < stages - 1)
        def _():
            back(i).wait_recv()

    def normed(i):
        wide = h_in[i].astype(F32)
        scale = lax.rsqrt(jnp.mean(wide * wide, -1, keepdims=True) + 1e-6)
        return wide, scale, (wide * scale).astype(BF16)

    def place(i):
        m, c = lax.div(i, pieces), lax.rem(i, pieces)
        return lax.rem(m, 2), lax.rem(m, act.shape[0]), pl.ds(pl.multiple_of(c * rows, rows), rows)

    def forward(i, start):
        wait_h(i)
        if not start:

            @pl.when(i >= RING)
            def _():
                onward(i - RING).wait_send()

        _, _, a = normed(i)
        spot = lax.rem(i, keeps)
        _, slot, here = place(jnp.where(first, i + 2 * pieces, i))
        for j in tiles:
            cols = pl.ds(j, COLS)
            if start:
                load_w(0, j).wait()
                load_w(1, j).wait()

            gate, up = dot(a, wg[:, cols]), dot(a, wu[:, cols])
            sg = jax.nn.sigmoid(gate)
            silu = gate * sg
            kept_s[spot, :, cols] = silu
            kept_q[spot, :, cols] = up * (sg + silu * (1.0 - sg))
            act[slot, here, cols] = (silu * up).astype(BF16)
        if start:
            for j in tiles:
                load_w(2, j).wait()

        y = dot(act[slot, here, :], wd[...]).astype(BF16)
        h_out[lax.rem(i, RING)] = h_in[i] + y
        onward(i).start()

    def backward(i, recompute, send):
        @pl.when(last)
        def _():
            wait_h(i)

        wait_d(i)
        slot, act_slot, here = place(i)
        spot = lax.rem(i, keeps)
        wide, scale, a = normed(i)
        by = d_in[i]
        at[slot, :, here] = a.T
        byt[slot, :, here] = by.T
        if recompute:
            for j in tiles:
                cols = pl.ds(j, COLS)
                gate, up = dot(a, wg[:, cols]), dot(a, wu[:, cols])
                by_act = dot(by, wdt[:, cols]).astype(BF16).astype(F32)
                sg = jax.nn.sigmoid(gate)
                silu = gate * sg
                act[act_slot, here, cols] = (silu * up).astype(BF16)
                du[slot, here, cols] = (by_act * silu).astype(BF16)
                dg[slot, here, cols] = (by_act * (up * (sg + silu * (1.0 - sg)))).astype(BF16)
            if send:
                by_a_g, by_a_u = dot(dg[slot, here, :], wgt[...]), dot(du[slot, here, :], wut[...])
        else:
            by_a_g, by_a_u = 0.0, 0.0
            firsts = [dot(by, wdt[:, pl.ds(j, COLS)]) for j in tiles]
            for j, by_act in zip(tiles, firsts, strict=True):
                cols = pl.ds(j, COLS)
                by_act = by_act.astype(BF16).astype(F32)
                by_up = (by_act * kept_s[spot, :, cols]).astype(BF16)
                by_gate = (by_act * kept_q[spot, :, cols]).astype(BF16)
                du[slot, here, cols] = by_up
                dg[slot, here, cols] = by_gate
                by_a_g += dot(by_gate, wgt[cols, :])
                by_a_u += dot(by_up, wut[cols, :])
        if send:
            by_a = (by_a_g.astype(BF16) + by_a_u.astype(BF16)).astype(F32)
            inner = jnp.sum(by_a * wide, -1, keepdims=True) * (scale * scale * scale) * (1.0 / d)
            d_in[i] = by + (by_a * scale - wide * inner).astype(BF16)
            back(i).start()

    jobs = [(k, j) for k in range(3) for j in tiles]
    sets = pieces // PARTS

    def weigh(m, p, e, final):
        slot, act_slot = lax.rem(m, 2), lax.rem(m, act.shape[0])
        here = pl.ds(pl.multiple_of(p * (d // PARTS), d // PARTS), d // PARTS)
        for k, j in jobs[e * len(jobs) // sets : (e + 1) * len(jobs) // sets]:
            cols = pl.ds(j, COLS)
            lhs = (at, at, byt)[k][slot, here, :]
            rhs = act[act_slot, :, cols] if k == 2 else (dg, du)[k][slot, :, cols]
            acc, out = (acc_g, acc_u, acc_d)[k], (wg, wu, wd)[k]
            total = acc[here, cols] + dot(lhs, rhs).astype(BF16).astype(F32)
            if not final:
                acc[here, cols] = total
            elif k == 2:
                out[cols, here] = total.astype(BF16).T
            else:
                out[here, cols] = total.astype(BF16)

    def step(i, carry):
        @pl.when(i == jnp.where(first, 3, 0))
        def _():
            for j in tiles:
                wdt[:, j : j + COLS] = wd[j : j + COLS, :].T
            for acc in (acc_g, acc_u, acc_d):
                acc[...] = jnp.zeros_like(acc)

            @pl.when(me > 0)
            def _():
                for j in tiles:
                    wgt[j : j + COLS, :] = wg[:, j : j + COLS].T
                    wut[j : j + COLS, :] = wu[:, j : j + COLS].T

        @pl.when(first & (i == 0))
        def _():
            forward(i, True)

        @pl.when((me < stages - 1) & (i + me > 0) & (i < n))
        def _():
            forward(i, False)

        ib = i - lag

        @pl.when((ib >= 0) & (ib < n) & middle)
        def _():
            backward(ib, False, True)

        @pl.when((ib >= 0) & (ib < n) & last)
        def _():
            backward(ib, True, True)

        @pl.when((ib >= 0) & (ib < n) & first)
        def _():
            backward(ib, True, False)

        iw = ib - pieces
        mw, pw = lax.div(iw, pieces), lax.div(lax.rem(iw, pieces), sets)
        for e in range(sets):
            turn = (iw >= 0) & (lax.rem(iw + pieces, sets) == e)

            @pl.when(turn & (iw < n - pieces))
            def _():
                weigh(mw, pw, e, False)

            @pl.when(turn & (iw >= n - pieces))
            def _():
                weigh(mw, pw, e, True)

        return carry

    lax.fori_loop(0, n + lag + pieces, step, 0)

    @pl.when(me < stages - 1)
    def _():
        lax.fori_loop(n - RING, n, lambda i, c: (onward(i).wait_send(), c)[1], 0)

    @pl.when(me > 0)
    def _():
        lax.fori_loop(0, n, lambda i, c: (back(i).wait_send(), c)[1], 0)


def solution(mesh):
    stages = mesh.shape["pp"]

    def step(x, dy, w_gate, w_up, w_down):
        micro, tokens, d = x.shape
        ff = w_gate.shape[2]
        pieces = tokens // ROWS
        n = micro * pieces
        chunks = lambda v: v.reshape(n, ROWS, d)
        vmem = lambda *shape, dtype=BF16: pltpu.VMEM(shape, dtype)
        sems = lambda *shape: pltpu.SemaphoreType.DMA(shape)
        og, ou, od = pl.pallas_call(
            functools.partial(kernel, stages, pieces),
            name="pipeline",
            out_shape=[pltpu.VMEM(shape, BF16) for shape in ((d, ff), (d, ff), (ff, d))],
            in_specs=[pl.BlockSpec(memory_space=pltpu.HBM)] * 5,
            out_specs=[pl.BlockSpec(memory_space=pltpu.VMEM)] * 3,
            scratch_shapes=[
                vmem(ff, d), vmem(ff, d), vmem(d, ff),
                *[vmem(d, ff, dtype=F32)] * 3,
                *[vmem(n, ROWS, d)] * 2,
                vmem(RING, ROWS, d),
                *[vmem(max(stages - 2, 0) * LAG + 1, ROWS, ff, dtype=F32)] * 2,
                vmem(4, tokens, ff), *[vmem(2, tokens, ff)] * 2,
                vmem(2, d, tokens), vmem(2, d, tokens),
                sems(3, ff // COLS), sems(n), sems(n), sems(n), sems(n),
            ],
            compiler_params=pltpu.CompilerParams(collective_id=0, has_side_effects=True, vmem_limit_bytes=61_500_000),
        )(chunks(x), chunks(dy), w_gate[0], w_up[0], w_down[0])
        return og[None], ou[None], od[None]

    return jax.shard_map(
        step,
        mesh=mesh,
        in_specs=(P("rep", None, None),) * 2 + (P("pp", None, None),) * 3,
        out_specs=(P(("rep", "pp"), None, None),) * 3,
        check_vma=False,
    )
```

```python
import functools

import jax
import jax.numpy as jnp
from jax import lax
from jax.experimental import pallas as pl
from jax.experimental.pallas import tpu as pltpu
from jax.sharding import PartitionSpec as P

ROWS = 128
PARTS = 2
COLS = 256
RING = 3
LAG = 4
MESH = pl.DeviceIdType.MESH
F32, BF16 = jnp.float32, jnp.bfloat16


def dot(a, b):
    return jnp.dot(a, b, preferred_element_type=F32)


def kernel(
    stages, pieces,
    x, dy, wg_in, wu_in, wd_in,
    wg, wu, wd,
    wgt, wut, wdt, acc_g, acc_u, acc_d,
    h_in, d_in, h_out, kept_s, kept_q, act, dg, du, at, byt,
    w_sem, rf, rb, sf, sb,
):
    me = lax.axis_index("pp")
    n, rows, d = x.shape
    ff = wg_in.shape[1]
    first, last = me == 0, me == stages - 1
    middle = (me > 0) & (me < stages - 1)
    keeps = kept_s.shape[0]
    lag = (stages - 1 - me) * LAG

    def load_x(i):
        return pltpu.make_async_copy(x.at[i], h_in.at[i], rf.at[i])

    def load_dy(i):
        return pltpu.make_async_copy(dy.at[i], d_in.at[i], rb.at[i])

    tiles = range(0, ff, COLS)

    def load_w(k, j):
        src, dst = ((wg_in, wg), (wu_in, wu), (wd_in, wd))[k]
        part = (pl.ds(j, COLS), slice(None)) if k == 2 else (slice(None), pl.ds(j, COLS))
        return pltpu.make_async_copy(src.at[part], dst.at[part], w_sem.at[k, j // COLS])

    @pl.when(first)
    def _():
        load_x(0).start()

    for j in tiles:
        load_w(0, j).start()
        load_w(1, j).start()
    for j in tiles:
        load_w(2, j).start()

    @pl.when(first)
    def _():
        lax.fori_loop(1, n, lambda i, c: (load_x(i).start(), c)[1], 0)

    @pl.when(last)
    def _():
        lax.fori_loop(0, n, lambda i, c: (load_dy(i).start(), c)[1], 0)

    def onward(i):
        return pltpu.make_async_remote_copy(
            src_ref=h_out.at[lax.rem(i, RING)], dst_ref=h_in.at[i], send_sem=sf.at[i], recv_sem=rf.at[i],
            device_id={"pp": jnp.minimum(me + 1, stages - 1)}, device_id_type=MESH,
        )

    def back(i):
        return pltpu.make_async_remote_copy(
            src_ref=d_in.at[i], dst_ref=d_in.at[i], send_sem=sb.at[i], recv_sem=rb.at[i],
            device_id={"pp": jnp.maximum(me - 1, 0)}, device_id_type=MESH,
        )

    barrier = pltpu.get_barrier_semaphore()

    @pl.when(me > 0)
    def _():
        pl.semaphore_signal(barrier, inc=1, device_id={"pp": me - 1}, device_id_type=MESH)

    @pl.when(me < stages - 1)
    def _():
        pl.semaphore_signal(barrier, inc=1, device_id={"pp": me + 1}, device_id_type=MESH)

    pl.semaphore_wait(barrier, (me > 0).astype(jnp.int32) + (me < stages - 1).astype(jnp.int32))

    @pl.when(me > 0)
    def _():
        for j in tiles:
            for k in range(3):
                load_w(k, j).wait()

    def wait_h(i):
        @pl.when(first)
        def _():
            load_x(i).wait()

        @pl.when(me > 0)
        def _():
            onward(i).wait_recv()

    def wait_d(i):
        @pl.when(last)
        def _():
            load_dy(i).wait()

        @pl.when(me < stages - 1)
        def _():
            back(i).wait_recv()

    def normed(i):
        wide = h_in[i].astype(F32)
        scale = lax.rsqrt(jnp.mean(wide * wide, -1, keepdims=True) + 1e-6)
        return wide, scale, (wide * scale).astype(BF16)

    def place(i):
        m, c = lax.div(i, pieces), lax.rem(i, pieces)
        return lax.rem(m, 2), lax.rem(m, act.shape[0]), pl.ds(pl.multiple_of(c * rows, rows), rows)

    def forward(i, start):
        wait_h(i)
        if not start:

            @pl.when(i >= RING)
            def _():
                onward(i - RING).wait_send()

        _, _, a = normed(i)
        spot = lax.rem(i, keeps)
        _, slot, here = place(jnp.where(first, i + 2 * pieces, i))
        for j in tiles:
            cols = pl.ds(j, COLS)
            if start:
                load_w(0, j).wait()
                load_w(1, j).wait()

            gate, up = dot(a, wg[:, cols]), dot(a, wu[:, cols])
            sg = jax.nn.sigmoid(gate)
            silu = gate * sg
            kept_s[spot, :, cols] = silu
            kept_q[spot, :, cols] = up * (sg + silu * (1.0 - sg))
            act[slot, here, cols] = (silu * up).astype(BF16)
        if start:
            for j in tiles:
                load_w(2, j).wait()

        y = dot(act[slot, here, :], wd[...]).astype(BF16)
        h_out[lax.rem(i, RING)] = h_in[i] + y
        onward(i).start()

    def backward(i, recompute, send):
        @pl.when(last)
        def _():
            wait_h(i)

        wait_d(i)
        slot, act_slot, here = place(i)
        spot = lax.rem(i, keeps)
        wide, scale, a = normed(i)
        by = d_in[i]
        at[slot, :, here] = a.T
        byt[slot, :, here] = by.T
        if recompute:
            for j in tiles:
                cols = pl.ds(j, COLS)
                gate, up = dot(a, wg[:, cols]), dot(a, wu[:, cols])
                by_act = dot(by, wdt[:, cols]).astype(BF16).astype(F32)
                sg = jax.nn.sigmoid(gate)
                silu = gate * sg
                act[act_slot, here, cols] = (silu * up).astype(BF16)
                du[slot, here, cols] = (by_act * silu).astype(BF16)
                dg[slot, here, cols] = (by_act * (up * (sg + silu * (1.0 - sg)))).astype(BF16)
            if send:
                by_a_g, by_a_u = dot(dg[slot, here, :], wgt[...]), dot(du[slot, here, :], wut[...])
        else:
            by_a_g, by_a_u = 0.0, 0.0
            firsts = [dot(by, wdt[:, pl.ds(j, COLS)]) for j in tiles]
            for j, by_act in zip(tiles, firsts, strict=True):
                cols = pl.ds(j, COLS)
                by_act = by_act.astype(BF16).astype(F32)
                by_up = (by_act * kept_s[spot, :, cols]).astype(BF16)
                by_gate = (by_act * kept_q[spot, :, cols]).astype(BF16)
                du[slot, here, cols] = by_up
                dg[slot, here, cols] = by_gate
                by_a_g += dot(by_gate, wgt[cols, :])
                by_a_u += dot(by_up, wut[cols, :])
        if send:
            by_a = (by_a_g.astype(BF16) + by_a_u.astype(BF16)).astype(F32)
            inner = jnp.sum(by_a * wide, -1, keepdims=True) * (scale * scale * scale) * (1.0 / d)
            d_in[i] = by + (by_a * scale - wide * inner).astype(BF16)
            back(i).start()

    jobs = [(k, j) for k in range(3) for j in tiles]
    sets = pieces // PARTS

    def weigh(m, p, e, final):
        slot, act_slot = lax.rem(m, 2), lax.rem(m, act.shape[0])
        here = pl.ds(pl.multiple_of(p * (d // PARTS), d // PARTS), d // PARTS)
        for k, j in jobs[e * len(jobs) // sets : (e + 1) * len(jobs) // sets]:
            cols = pl.ds(j, COLS)
            lhs = (at, at, byt)[k][slot, here, :]
            rhs = act[act_slot, :, cols] if k == 2 else (dg, du)[k][slot, :, cols]
            acc, out = (acc_g, acc_u, acc_d)[k], (wg, wu, wd)[k]
            total = acc[here, cols] + dot(lhs, rhs).astype(BF16).astype(F32)
            if not final:
                acc[here, cols] = total
            elif k == 2:
                out[cols, here] = total.astype(BF16).T
            else:
                out[here, cols] = total.astype(BF16)

    def weigh_half(h):
        m, half = n // pieces - 1, pieces * rows // 2
        part, slots = pl.ds(h * half, half), d // rows
        for k, j in sorted(jobs, reverse=True):
            cols = pl.ds(j, COLS)
            left = (at, at, byt)[k].at[m % 2]
            right = act.at[m % act.shape[0]] if k == 2 else (dg, du)[k].at[m % 2]
            acc, out = (acc_g, acc_u, acc_d)[k], (wg, wu, wd)[k]
            kept, first_spot = (kept_s, kept_s, kept_q)[k], (0, slots, 0)[k]
            for p in range(0, d, d // PARTS):
                term = dot(left[pl.ds(p, d // PARTS), part], right[part, cols])
                for r in range(0, d // PARTS, rows):
                    here, spot, one = pl.ds(p + r, rows), first_spot + (p + r) // rows, term[r : r + rows]
                    if h == 0:
                        kept[spot, :, cols] = one
                    else:
                        one = (kept[spot, :, cols] + one).astype(BF16).astype(F32)
                        total = (acc[here, cols] + one).astype(BF16)
                        if k == 2:
                            out[cols, here] = total.T
                        else:
                            out[here, cols] = total

    def step(i, carry):
        @pl.when(i == jnp.where(first, 3, 0))
        def _():
            for j in tiles:
                wdt[:, j : j + COLS] = wd[j : j + COLS, :].T
            for acc in (acc_g, acc_u, acc_d):
                acc[...] = jnp.zeros_like(acc)

            @pl.when(me > 0)
            def _():
                for j in tiles:
                    wgt[j : j + COLS, :] = wg[:, j : j + COLS].T
                    wut[j : j + COLS, :] = wu[:, j : j + COLS].T

        @pl.when(first & (i == 0))
        def _():
            forward(i, True)

        @pl.when((me < stages - 1) & (i + me > 0) & (i < n))
        def _():
            forward(i, False)

        ib = i - lag

        @pl.when((ib >= 0) & (ib < n) & middle)
        def _():
            backward(ib, False, True)

        @pl.when((ib >= 0) & (ib < n) & last)
        def _():
            backward(ib, True, True)

        @pl.when((ib >= 0) & (ib < n) & first)
        def _():
            backward(ib, True, False)

        hurry = first & (ib >= n - pieces)
        start = jnp.where(hurry, n - 2 * pieces + 2 * (ib - n + pieces), ib - pieces)
        count = jnp.where(hurry, jnp.where(ib < n - pieces // 2, 2, 0), jnp.where(ib >= pieces, 1, 0))

        def weigh_part(iw, carry):
            mw, pw = lax.div(iw, pieces), lax.div(lax.rem(iw, pieces), sets)
            for e in range(sets):
                turn = lax.rem(iw, sets) == e

                @pl.when(turn & (iw < n - pieces))
                def _():
                    weigh(mw, pw, e, False)

                @pl.when(turn & (iw >= n - pieces))
                def _():
                    weigh(mw, pw, e, True)

            return carry

        lax.fori_loop(start, start + count, weigh_part, 0)

        @pl.when(first & (ib == n - pieces // 2))
        def _():
            weigh_half(0)

        @pl.when(first & (ib == n - 1))
        def _():
            weigh_half(1)

        return carry

    lax.fori_loop(0, n + lag + jnp.where(first, 0, pieces), step, 0)

    @pl.when(me < stages - 1)
    def _():
        lax.fori_loop(n - RING, n, lambda i, c: (onward(i).wait_send(), c)[1], 0)

    @pl.when(me > 0)
    def _():
        lax.fori_loop(0, n, lambda i, c: (back(i).wait_send(), c)[1], 0)


def solution(mesh):
    stages = mesh.shape["pp"]

    def step(x, dy, w_gate, w_up, w_down):
        micro, tokens, d = x.shape
        ff = w_gate.shape[2]
        pieces = tokens // ROWS
        n = micro * pieces
        chunks = lambda v: v.reshape(n, ROWS, d)
        vmem = lambda *shape, dtype=BF16: pltpu.VMEM(shape, dtype)
        sems = lambda *shape: pltpu.SemaphoreType.DMA(shape)
        og, ou, od = pl.pallas_call(
            functools.partial(kernel, stages, pieces),
            name="pipeline",
            out_shape=[pltpu.VMEM(shape, BF16) for shape in ((d, ff), (d, ff), (ff, d))],
            in_specs=[pl.BlockSpec(memory_space=pltpu.HBM)] * 5,
            out_specs=[pl.BlockSpec(memory_space=pltpu.VMEM)] * 3,
            scratch_shapes=[
                vmem(ff, d), vmem(ff, d), vmem(d, ff),
                *[vmem(d, ff, dtype=F32)] * 3,
                *[vmem(n, ROWS, d)] * 2,
                vmem(RING, ROWS, d),
                *[vmem(max(stages - 2, 0) * LAG + 1, ROWS, ff, dtype=F32)] * 2,
                vmem(4, tokens, ff), *[vmem(2, tokens, ff)] * 2,
                vmem(2, d, tokens), vmem(2, d, tokens),
                sems(3, ff // COLS), sems(n), sems(n), sems(n), sems(n),
            ],
            compiler_params=pltpu.CompilerParams(collective_id=0, has_side_effects=True, vmem_limit_bytes=61_500_000),
        )(chunks(x), chunks(dy), w_gate[0], w_up[0], w_down[0])
        return og[None], ou[None], od[None]

    return jax.shard_map(
        step,
        mesh=mesh,
        in_specs=(P("rep", None, None),) * 2 + (P("pp", None, None),) * 3,
        out_specs=(P(("rep", "pp"), None, None),) * 3,
        check_vma=False,
    )
```

```python
import functools

import jax
import jax.numpy as jnp
from jax import lax
from jax.experimental import pallas as pl
from jax.experimental.pallas import tpu as pltpu
from jax.sharding import PartitionSpec as P

ROWS = 128
PARTS = 2
COLS = 256
RING = 3
LAG = 4
MESH = pl.DeviceIdType.MESH
F32, BF16 = jnp.float32, jnp.bfloat16


def dot(a, b):
    return jnp.dot(a, b, preferred_element_type=F32)


def kernel(
    stages, pieces,
    x, dy, wg_in, wu_in, wd_in,
    wg, wu, wd,
    wgt, wut, wdt, acc_g, acc_u, acc_d,
    h_in, d_in, h_out, kept_s, kept_q, act, dg, du, at, byt,
    w_sem, rf, rb, sf, sb,
):
    me = lax.axis_index("pp")
    n, rows, d = x.shape
    ff = wg_in.shape[1]
    first, last = me == 0, me == stages - 1
    middle = (me > 0) & (me < stages - 1)
    keeps = kept_s.shape[0]
    lag = (stages - 1 - me) * LAG

    def load_x(i):
        return pltpu.make_async_copy(x.at[i], h_in.at[i], rf.at[i])

    def load_dy(i):
        return pltpu.make_async_copy(dy.at[i], d_in.at[i], rb.at[i])

    tiles = range(0, ff, COLS)

    def load_w(k, j):
        src, dst = ((wg_in, wg), (wu_in, wu), (wd_in, wd))[k]
        part = (pl.ds(j, COLS), slice(None)) if k == 2 else (slice(None), pl.ds(j, COLS))
        return pltpu.make_async_copy(src.at[part], dst.at[part], w_sem.at[k, j // COLS])

    @pl.when(first)
    def _():
        load_x(0).start()

    for j in tiles:
        load_w(0, j).start()
        load_w(1, j).start()
    for j in tiles:
        load_w(2, j).start()

    @pl.when(first)
    def _():
        lax.fori_loop(1, n, lambda i, c: (load_x(i).start(), c)[1], 0)

    @pl.when(last)
    def _():
        lax.fori_loop(0, n, lambda i, c: (load_dy(i).start(), c)[1], 0)

    def onward(i):
        return pltpu.make_async_remote_copy(
            src_ref=h_out.at[lax.rem(i, RING)], dst_ref=h_in.at[i], send_sem=sf.at[i], recv_sem=rf.at[i],
            device_id={"pp": jnp.minimum(me + 1, stages - 1)}, device_id_type=MESH,
        )

    def back(i):
        return pltpu.make_async_remote_copy(
            src_ref=d_in.at[i], dst_ref=d_in.at[i], send_sem=sb.at[i], recv_sem=rb.at[i],
            device_id={"pp": jnp.maximum(me - 1, 0)}, device_id_type=MESH,
        )

    barrier = pltpu.get_barrier_semaphore()

    @pl.when(me > 0)
    def _():
        pl.semaphore_signal(barrier, inc=1, device_id={"pp": me - 1}, device_id_type=MESH)

    @pl.when(me < stages - 1)
    def _():
        pl.semaphore_signal(barrier, inc=1, device_id={"pp": me + 1}, device_id_type=MESH)

    pl.semaphore_wait(barrier, (me > 0).astype(jnp.int32) + (me < stages - 1).astype(jnp.int32))

    @pl.when(me > 0)
    def _():
        for j in tiles:
            for k in range(3):
                load_w(k, j).wait()

    def wait_h(i):
        @pl.when(first)
        def _():
            load_x(i).wait()

        @pl.when(me > 0)
        def _():
            onward(i).wait_recv()

    def wait_d(i):
        @pl.when(last)
        def _():
            load_dy(i).wait()

        @pl.when(me < stages - 1)
        def _():
            back(i).wait_recv()

    def normed(i):
        wide = h_in[i].astype(F32)
        scale = lax.rsqrt(jnp.mean(wide * wide, -1, keepdims=True) + 1e-6)
        return wide, scale, (wide * scale).astype(BF16)

    def place(i):
        m, c = lax.div(i, pieces), lax.rem(i, pieces)
        return lax.rem(m, 2), lax.rem(m, act.shape[0]), pl.ds(pl.multiple_of(c * rows, rows), rows)

    def forward(i, start):
        wait_h(i)
        if not start:

            @pl.when(i >= RING)
            def _():
                onward(i - RING).wait_send()

        _, _, a = normed(i)
        spot = lax.rem(i, keeps)
        _, slot, here = place(jnp.where(first, i + 2 * pieces, i))
        for j in tiles:
            cols = pl.ds(j, COLS)
            if start:
                load_w(0, j).wait()
                load_w(1, j).wait()

            gate, up = dot(a, wg[:, cols]), dot(a, wu[:, cols])
            sg = jax.nn.sigmoid(gate)
            silu = gate * sg
            kept_s[spot, :, cols] = silu
            kept_q[spot, :, cols] = up * (sg + silu * (1.0 - sg))
            act[slot, here, cols] = (silu * up).astype(BF16)
        if start:
            for j in tiles:
                load_w(2, j).wait()

        y = dot(act[slot, here, :], wd[...]).astype(BF16)
        h_out[lax.rem(i, RING)] = h_in[i] + y
        onward(i).start()
        if not start:
            @pl.when(first & (i == n - 1))
            def _():
                kept_q[keeps - 1] = act[slot, here, :].astype(F32)

    def backward(i, recompute, send):
        @pl.when(last)
        def _():
            wait_h(i)

        wait_d(i)
        slot, act_slot, here = place(i)
        spot = lax.rem(i, keeps)
        wide, scale, a = normed(i)
        by = d_in[i]
        at[slot, :, here] = a.T
        byt[slot, :, here] = by.T
        if recompute:
            for j in tiles:
                cols = pl.ds(j, COLS)
                gate, up = dot(a, wg[:, cols]), dot(a, wu[:, cols])
                by_act = dot(by, wdt[:, cols]).astype(BF16).astype(F32)
                sg = jax.nn.sigmoid(gate)
                silu = gate * sg
                act[act_slot, here, cols] = (silu * up).astype(BF16)
                du[slot, here, cols] = (by_act * silu).astype(BF16)
                dg[slot, here, cols] = (by_act * (up * (sg + silu * (1.0 - sg)))).astype(BF16)
        else:
            for j in tiles:
                cols = pl.ds(j, COLS)
                by_act = dot(by, wdt[:, cols]).astype(BF16).astype(F32)
                du[slot, here, cols] = (by_act * kept_s[spot, :, cols]).astype(BF16)
                dg[slot, here, cols] = (by_act * kept_q[spot, :, cols]).astype(BF16)
                if not send:
                    act[act_slot, here, cols] = kept_q[keeps - 1, :, cols].astype(BF16)
        if send:
            by_a_g, by_a_u = dot(dg[slot, here, :], wgt[...]), dot(du[slot, here, :], wut[...])
            by_a = (by_a_g.astype(BF16) + by_a_u.astype(BF16)).astype(F32)
            inner = jnp.sum(by_a * wide, -1, keepdims=True) * (scale * scale * scale) * (1.0 / d)
            d_in[i] = by + (by_a * scale - wide * inner).astype(BF16)
            back(i).start()

    jobs = [(k, j) for k in range(3) for j in tiles]
    sets = pieces // PARTS

    def weigh(m, p, e, final):
        slot, act_slot = lax.rem(m, 2), lax.rem(m, act.shape[0])
        here = pl.ds(pl.multiple_of(p * (d // PARTS), d // PARTS), d // PARTS)
        for k, j in jobs[e * len(jobs) // sets : (e + 1) * len(jobs) // sets]:
            cols = pl.ds(j, COLS)
            lhs = (at, at, byt)[k][slot, here, :]
            rhs = act[act_slot, :, cols] if k == 2 else (dg, du)[k][slot, :, cols]
            acc, out = (acc_g, acc_u, acc_d)[k], (wg, wu, wd)[k]
            total = acc[here, cols] + dot(lhs, rhs).astype(BF16).astype(F32)
            if not final:
                acc[here, cols] = total
            elif k == 2:
                out[cols, here] = total.astype(BF16).T
            else:
                out[here, cols] = total.astype(BF16)

    def weigh_half(h):
        m, half = n // pieces - 1, pieces * rows // 2
        part, slots = pl.ds(h * half, half), d // rows
        for k, j in sorted(jobs, reverse=True):
            cols = pl.ds(j, COLS)
            left = (at, at, byt)[k].at[m % 2]
            right = act.at[m % act.shape[0]] if k == 2 else (dg, du)[k].at[m % 2]
            acc, out = (acc_g, acc_u, acc_d)[k], (wg, wu, wd)[k]
            kept, first_spot = (kept_s, kept_s, kept_q)[k], (0, slots, 0)[k]
            taken = (n - 1) % keeps
            for p in range(0, d, d // PARTS):
                term = dot(left[pl.ds(p, d // PARTS), part], right[part, cols])
                for r in range(0, d // PARTS, rows):
                    here, spot, one = pl.ds(p + r, rows), first_spot + (p + r) // rows, term[r : r + rows]
                    spot += spot >= taken
                    if h == 0:
                        kept[spot, :, cols] = one
                    else:
                        one = (kept[spot, :, cols] + one).astype(BF16).astype(F32)
                        total = (acc[here, cols] + one).astype(BF16)
                        if k == 2:
                            out[cols, here] = total.T
                        else:
                            out[here, cols] = total

    def step(i, carry):
        @pl.when(i == jnp.where(first, 3, 0))
        def _():
            for j in tiles:
                wdt[:, j : j + COLS] = wd[j : j + COLS, :].T
            for acc in (acc_g, acc_u, acc_d):
                acc[...] = jnp.zeros_like(acc)

            @pl.when(me > 0)
            def _():
                for j in tiles:
                    wgt[j : j + COLS, :] = wg[:, j : j + COLS].T
                    wut[j : j + COLS, :] = wu[:, j : j + COLS].T

        @pl.when(first & (i == 0))
        def _():
            forward(i, True)

        @pl.when((me < stages - 1) & (i + me > 0) & (i < n))
        def _():
            forward(i, False)

        ib = i - lag

        @pl.when((ib >= 0) & (ib < n) & middle)
        def _():
            backward(ib, False, True)

        @pl.when((ib >= 0) & (ib < n) & last)
        def _():
            backward(ib, True, True)

        @pl.when((ib >= 0) & (ib < n - 1) & first)
        def _():
            backward(ib, True, False)

        @pl.when((ib == n - 1) & first)
        def _():
            backward(ib, False, False)

        hurry = first & (ib >= n - pieces)
        start = jnp.where(hurry, n - 2 * pieces + 2 * (ib - n + pieces), ib - pieces)
        count = jnp.where(hurry, jnp.where(ib < n - pieces // 2, 2, 0), jnp.where(ib >= pieces, 1, 0))

        def weigh_part(iw, carry):
            mw, pw = lax.div(iw, pieces), lax.div(lax.rem(iw, pieces), sets)
            for e in range(sets):
                turn = lax.rem(iw, sets) == e

                @pl.when(turn & (iw < n - pieces))
                def _():
                    weigh(mw, pw, e, False)

                @pl.when(turn & (iw >= n - pieces))
                def _():
                    weigh(mw, pw, e, True)

            return carry

        lax.fori_loop(start, start + count, weigh_part, 0)

        @pl.when(first & (ib == n - pieces // 2))
        def _():
            weigh_half(0)

        @pl.when(first & (ib == n - 1))
        def _():
            weigh_half(1)

        return carry

    lax.fori_loop(0, n + lag + jnp.where(first, 0, pieces), step, 0)

    @pl.when(me < stages - 1)
    def _():
        lax.fori_loop(n - RING, n, lambda i, c: (onward(i).wait_send(), c)[1], 0)

    @pl.when(me > 0)
    def _():
        lax.fori_loop(0, n, lambda i, c: (back(i).wait_send(), c)[1], 0)


def solution(mesh):
    stages = mesh.shape["pp"]

    def step(x, dy, w_gate, w_up, w_down):
        micro, tokens, d = x.shape
        ff = w_gate.shape[2]
        pieces = tokens // ROWS
        n = micro * pieces
        chunks = lambda v: v.reshape(n, ROWS, d)
        vmem = lambda *shape, dtype=BF16: pltpu.VMEM(shape, dtype)
        sems = lambda *shape: pltpu.SemaphoreType.DMA(shape)
        og, ou, od = pl.pallas_call(
            functools.partial(kernel, stages, pieces),
            name="pipeline",
            out_shape=[pltpu.VMEM(shape, BF16) for shape in ((d, ff), (d, ff), (ff, d))],
            in_specs=[pl.BlockSpec(memory_space=pltpu.HBM)] * 5,
            out_specs=[pl.BlockSpec(memory_space=pltpu.VMEM)] * 3,
            scratch_shapes=[
                vmem(ff, d), vmem(ff, d), vmem(d, ff),
                *[vmem(d, ff, dtype=F32)] * 3,
                *[vmem(n, ROWS, d)] * 2,
                vmem(RING, ROWS, d),
                *[vmem(max(stages - 2, 0) * LAG + 1, ROWS, ff, dtype=F32)] * 2,
                vmem(4, tokens, ff), *[vmem(2, tokens, ff)] * 2,
                vmem(2, d, tokens), vmem(2, d, tokens),
                sems(3, ff // COLS), sems(n), sems(n), sems(n), sems(n),
            ],
            compiler_params=pltpu.CompilerParams(collective_id=0, has_side_effects=True, vmem_limit_bytes=61_500_000),
        )(chunks(x), chunks(dy), w_gate[0], w_up[0], w_down[0])
        return og[None], ou[None], od[None]

    return jax.shard_map(
        step,
        mesh=mesh,
        in_specs=(P("rep", None, None),) * 2 + (P("pp", None, None),) * 3,
        out_specs=(P(("rep", "pp"), None, None),) * 3,
        check_vma=False,
    )
```

```python
import functools

import jax
import jax.numpy as jnp
from jax import lax
from jax.experimental import pallas as pl
from jax.experimental.pallas import tpu as pltpu
from jax.sharding import PartitionSpec as P

ROWS = 128
PARTS = 2
COLS = 256
RING = 3
LAG = 4
MESH = pl.DeviceIdType.MESH
F32, BF16 = jnp.float32, jnp.bfloat16


def dot(a, b):
    return jnp.dot(a, b, preferred_element_type=F32)


def kernel(
    stages, pieces,
    x, dy, wg_in, wu_in, wd_in,
    wg, wu, wd,
    wgt, wut, wdt, acc_g, acc_u, acc_d,
    h_in, d_in, h_out, kept_s, kept_q, act, dg, du, at, byt,
    w_sem, rf, rb, sf, sb,
):
    me = lax.axis_index("pp")
    n, rows, d = x.shape
    ff = wg_in.shape[1]
    first, last = me == 0, me == stages - 1
    middle = (me > 0) & (me < stages - 1)
    keeps = kept_s.shape[0]
    lag = (stages - 1 - me) * LAG + jnp.where(first, 2, 0)

    def load_x(i):
        return pltpu.make_async_copy(x.at[i], h_in.at[i], rf.at[i])

    def load_dy(i):
        return pltpu.make_async_copy(dy.at[i], d_in.at[i], rb.at[i])

    tiles = range(0, ff, COLS)

    def load_w(k, j):
        src, dst = ((wg_in, wg), (wu_in, wu), (wd_in, wd))[k]
        part = (pl.ds(j, COLS), slice(None)) if k == 2 else (slice(None), pl.ds(j, COLS))
        return pltpu.make_async_copy(src.at[part], dst.at[part], w_sem.at[k, j // COLS])

    @pl.when(first)
    def _():
        load_x(0).start()
        load_x(1).start()

    for j in tiles:
        load_w(0, j).start()
        load_w(1, j).start()
    for j in tiles:
        load_w(2, j).start()

    @pl.when(last)
    def _():
        lax.fori_loop(0, n, lambda i, c: (load_dy(i).start(), c)[1], 0)

    def onward(i):
        return pltpu.make_async_remote_copy(
            src_ref=h_out.at[lax.rem(i, RING)], dst_ref=h_in.at[i], send_sem=sf.at[i], recv_sem=rf.at[i],
            device_id={"pp": jnp.minimum(me + 1, stages - 1)}, device_id_type=MESH,
        )

    def back(i):
        return pltpu.make_async_remote_copy(
            src_ref=d_in.at[i], dst_ref=d_in.at[i], send_sem=sb.at[i], recv_sem=rb.at[i],
            device_id={"pp": jnp.maximum(me - 1, 0)}, device_id_type=MESH,
        )

    barrier = pltpu.get_barrier_semaphore()

    @pl.when(me > 0)
    def _():
        pl.semaphore_signal(barrier, inc=1, device_id={"pp": me - 1}, device_id_type=MESH)

    @pl.when(me < stages - 1)
    def _():
        pl.semaphore_signal(barrier, inc=1, device_id={"pp": me + 1}, device_id_type=MESH)

    pl.semaphore_wait(barrier, (me > 0).astype(jnp.int32) + (me < stages - 1).astype(jnp.int32))

    @pl.when(me > 0)
    def _():
        for j in tiles:
            for k in range(3):
                load_w(k, j).wait()

    def wait_h(i):
        @pl.when(first)
        def _():
            load_x(i).wait()

        @pl.when(me > 0)
        def _():
            onward(i).wait_recv()

    def wait_d(i):
        @pl.when(last)
        def _():
            load_dy(i).wait()

        @pl.when(me < stages - 1)
        def _():
            back(i).wait_recv()

    def normed(i):
        wide = h_in[i].astype(F32)
        scale = lax.rsqrt(jnp.mean(wide * wide, -1, keepdims=True) + 1e-6)
        return wide, scale, (wide * scale).astype(BF16)

    def place(i):
        m, c = lax.div(i, pieces), lax.rem(i, pieces)
        return lax.rem(m, 2), lax.rem(m, act.shape[0]), pl.ds(pl.multiple_of(c * rows, rows), rows)

    def forward(i, start):
        wait_h(i)
        if not start:

            @pl.when(i >= RING)
            def _():
                onward(i - RING).wait_send()

        _, _, a = normed(i)
        spot = lax.rem(i, keeps)
        _, slot, here = place(jnp.where(first, i + 2 * pieces, i))
        for j in tiles:
            cols = pl.ds(j, COLS)
            if start:
                load_w(0, j).wait()
                load_w(1, j).wait()

            gate, up = dot(a, wg[:, cols]), dot(a, wu[:, cols])
            sg = jax.nn.sigmoid(gate)
            silu = gate * sg
            kept_s[spot, :, cols] = silu
            kept_q[spot, :, cols] = up * (sg + silu * (1.0 - sg))
            act[slot, here, cols] = (silu * up).astype(BF16)
        if start:
            for j in tiles:
                load_w(2, j).wait()

        y = dot(act[slot, here, :], wd[...]).astype(BF16)
        h_out[lax.rem(i, RING)] = h_in[i] + y
        onward(i).start()
        if not start:
            @pl.when(first & (i == n - 1))
            def _():
                kept_q[keeps - 1] = act[slot, here, :].astype(F32)

    def backward(i, recompute, send):
        @pl.when(last)
        def _():
            wait_h(i)

        wait_d(i)
        slot, act_slot, here = place(i)
        spot = lax.rem(i, keeps)
        wide, scale, a = normed(i)
        by = d_in[i]
        at[slot, :, here] = a.T
        byt[slot, :, here] = by.T
        if recompute:
            for j in tiles:
                cols = pl.ds(j, COLS)
                gate, up = dot(a, wg[:, cols]), dot(a, wu[:, cols])
                by_act = dot(by, wdt[:, cols]).astype(BF16).astype(F32)
                sg = jax.nn.sigmoid(gate)
                silu = gate * sg
                act[act_slot, here, cols] = (silu * up).astype(BF16)
                du[slot, here, cols] = (by_act * silu).astype(BF16)
                dg[slot, here, cols] = (by_act * (up * (sg + silu * (1.0 - sg)))).astype(BF16)
        else:
            for j in tiles:
                cols = pl.ds(j, COLS)
                by_act = dot(by, wdt[:, cols]).astype(BF16).astype(F32)
                du[slot, here, cols] = (by_act * kept_s[spot, :, cols]).astype(BF16)
                dg[slot, here, cols] = (by_act * kept_q[spot, :, cols]).astype(BF16)
                if not send:
                    act[act_slot, here, cols] = kept_q[keeps - 1, :, cols].astype(BF16)
        if send:
            by_a_g, by_a_u = dot(dg[slot, here, :], wgt[...]), dot(du[slot, here, :], wut[...])
            by_a = (by_a_g.astype(BF16) + by_a_u.astype(BF16)).astype(F32)
            inner = jnp.sum(by_a * wide, -1, keepdims=True) * (scale * scale * scale) * (1.0 / d)
            d_in[i] = by + (by_a * scale - wide * inner).astype(BF16)
            back(i).start()

    jobs = [(k, j) for k in range(3) for j in tiles]
    sets = pieces // PARTS

    def weigh(m, p, e, final):
        slot, act_slot = lax.rem(m, 2), lax.rem(m, act.shape[0])
        here = pl.ds(pl.multiple_of(p * (d // PARTS), d // PARTS), d // PARTS)
        for k, j in jobs[e * len(jobs) // sets : (e + 1) * len(jobs) // sets]:
            cols = pl.ds(j, COLS)
            lhs = (at, at, byt)[k][slot, here, :]
            rhs = act[act_slot, :, cols] if k == 2 else (dg, du)[k][slot, :, cols]
            acc, out = (acc_g, acc_u, acc_d)[k], (wg, wu, wd)[k]
            total = acc[here, cols] + dot(lhs, rhs).astype(BF16).astype(F32)
            if not final:
                acc[here, cols] = total
            elif k == 2:
                out[cols, here] = total.astype(BF16).T
            else:
                out[here, cols] = total.astype(BF16)

    def weigh_half(h):
        m, half = n // pieces - 1, pieces * rows // 2
        part, slots = pl.ds(h * half, half), d // rows
        for k, j in sorted(jobs, reverse=True):
            cols = pl.ds(j, COLS)
            left = (at, at, byt)[k].at[m % 2]
            right = act.at[m % act.shape[0]] if k == 2 else (dg, du)[k].at[m % 2]
            acc, out = (acc_g, acc_u, acc_d)[k], (wg, wu, wd)[k]
            kept, first_spot = (kept_s, kept_s, kept_q)[k], (0, slots, 0)[k]
            taken = (n - 1) % keeps
            for p in range(0, d, d // PARTS):
                term = dot(left[pl.ds(p, d // PARTS), part], right[part, cols])
                for r in range(0, d // PARTS, rows):
                    here, spot, one = pl.ds(p + r, rows), first_spot + (p + r) // rows, term[r : r + rows]
                    spot += spot >= taken
                    if h == 0:
                        kept[spot, :, cols] = one
                    else:
                        one = (kept[spot, :, cols] + one).astype(BF16).astype(F32)
                        total = (acc[here, cols] + one).astype(BF16)
                        if k == 2:
                            out[cols, here] = total.T
                        else:
                            out[here, cols] = total

    def step(i, carry):
        @pl.when(i == jnp.where(first, 3, 0))
        def _():
            for j in tiles:
                wdt[:, j : j + COLS] = wd[j : j + COLS, :].T
            for acc in (acc_g, acc_u, acc_d):
                acc[...] = jnp.zeros_like(acc)

            @pl.when(me > 0)
            def _():
                for j in tiles:
                    wgt[j : j + COLS, :] = wg[:, j : j + COLS].T
                    wut[j : j + COLS, :] = wu[:, j : j + COLS].T

        @pl.when(first & (i == 0))
        def _():
            forward(i, True)
            lax.fori_loop(2, n, lambda i, c: (load_x(i).start(), c)[1], 0)

        @pl.when((me < stages - 1) & (i + me > 0) & (i < n))
        def _():
            forward(i, False)

        ib = i - lag

        @pl.when((ib >= 0) & (ib < n) & middle)
        def _():
            backward(ib, False, True)

        @pl.when((ib >= 0) & (ib < n) & last)
        def _():
            backward(ib, True, True)

        @pl.when((ib >= 0) & (ib < n - 1) & first)
        def _():
            backward(ib, True, False)

        @pl.when((ib == n - 1) & first)
        def _():
            backward(ib, False, False)

        hurry = first & (ib >= n - pieces)
        start = jnp.where(hurry, n - 2 * pieces + 2 * (ib - n + pieces), ib - pieces)
        count = jnp.where(hurry, jnp.where(ib < n - pieces // 2, 2, 0), jnp.where(ib >= pieces, 1, 0))

        def weigh_part(iw, carry):
            mw, pw = lax.div(iw, pieces), lax.div(lax.rem(iw, pieces), sets)
            for e in range(sets):
                turn = lax.rem(iw, sets) == e

                @pl.when(turn & (iw < n - pieces))
                def _():
                    weigh(mw, pw, e, False)

                @pl.when(turn & (iw >= n - pieces))
                def _():
                    weigh(mw, pw, e, True)

            return carry

        lax.fori_loop(start, start + count, weigh_part, 0)

        @pl.when(first & (ib == n - pieces // 2))
        def _():
            weigh_half(0)

        @pl.when(first & (ib == n - 1))
        def _():
            weigh_half(1)

        return carry

    lax.fori_loop(0, n + lag + jnp.where(first, 0, pieces), step, 0)

    @pl.when(me < stages - 1)
    def _():
        lax.fori_loop(n - RING, n, lambda i, c: (onward(i).wait_send(), c)[1], 0)

    @pl.when(me > 0)
    def _():
        lax.fori_loop(0, n, lambda i, c: (back(i).wait_send(), c)[1], 0)


def solution(mesh):
    stages = mesh.shape["pp"]

    def step(x, dy, w_gate, w_up, w_down):
        micro, tokens, d = x.shape
        ff = w_gate.shape[2]
        pieces = tokens // ROWS
        n = micro * pieces
        chunks = lambda v: v.reshape(n, ROWS, d)
        vmem = lambda *shape, dtype=BF16: pltpu.VMEM(shape, dtype)
        sems = lambda *shape: pltpu.SemaphoreType.DMA(shape)
        og, ou, od = pl.pallas_call(
            functools.partial(kernel, stages, pieces),
            name="pipeline",
            out_shape=[pltpu.VMEM(shape, BF16) for shape in ((d, ff), (d, ff), (ff, d))],
            in_specs=[pl.BlockSpec(memory_space=pltpu.HBM)] * 5,
            out_specs=[pl.BlockSpec(memory_space=pltpu.VMEM)] * 3,
            scratch_shapes=[
                vmem(ff, d), vmem(ff, d), vmem(d, ff),
                *[vmem(d, ff, dtype=F32)] * 3,
                *[vmem(n, ROWS, d)] * 2,
                vmem(RING, ROWS, d),
                *[vmem(max(stages - 2, 0) * LAG + 1, ROWS, ff, dtype=F32)] * 2,
                vmem(4, tokens, ff), *[vmem(2, tokens, ff)] * 2,
                vmem(2, d, tokens), vmem(2, d, tokens),
                sems(3, ff // COLS), sems(n), sems(n), sems(n), sems(n),
            ],
            compiler_params=pltpu.CompilerParams(collective_id=0, has_side_effects=True, vmem_limit_bytes=61_500_000),
        )(chunks(x), chunks(dy), w_gate[0], w_up[0], w_down[0])
        return og[None], ou[None], od[None]

    return jax.shard_map(
        step,
        mesh=mesh,
        in_specs=(P("rep", None, None),) * 2 + (P("pp", None, None),) * 3,
        out_specs=(P(("rep", "pp"), None, None),) * 3,
        check_vma=False,
    )
```
